32 devices in a mesh: seq: 16 (over z, x, core), zero: 2 (over y).
Axes of the slice: x: 2, y: 2, z: 4, core: 2. Of those that a mesh axis runs over, the one named last changes fastest.
Arguments:
- tokens: bfloat16 [2, 2048, 2048], P('zero', 'seq'), may hold values from -6 to 6
- w_in: bfloat16 [2048, 2336], P('zero'), may hold values from -0.0625 to 0.0625
- a_log: float32 [32], replicated, may hold values from -8 to 0
- dt_bias: float32 [32], replicated, may hold values from -4.5 to -3.5
- d_skip: float32 [32], replicated, may hold values from 0.5 to 1.5
- grad_y: bfloat16 [2, 2048, 2048], P('zero', 'seq'), may hold values from -6 to 6
Outputs:
- y_out: bfloat16 [2, 2048, 2048], P('zero', 'seq')
- grad_tokens: bfloat16 [2, 2048, 2048], P('zero', 'seq')
- grad_w: float32 [2048, 2336], P(('seq', 'zero'))
The draws below stay inside these ranges and needn't reach their ends.
All inputs are finite; a program needn't handle non-finite values.
Results may differ from the reference program's by a relative error of at most 0.013.
Values may be sent and summed in bfloat16 or wider, within the bound.
A program may use at most 128 MiB of HBM per device.

```python
import jax
import jax.numpy as jnp
from jax import lax

D = 2048
STATE = 128
HEADS = 32
HEAD_SIZE = 64
TOK_DEV = 128
INNER = 2048
PROJ = 2336
BATCH = 2
LENGTH = 2048
N_SEQ = 16


def block_scale(own_key, extent, shards, least, top_value):
    level, own = 1.0, jax.random.fold_in(own_key, 6)
    for axis_at, shards_of in shards:
        draws = jnp.exp(jax.random.uniform(jax.random.fold_in(own, axis_at), (shards_of,), jnp.float32, least / len(shards), top_value / len(shards)))
        level = level * jnp.repeat(draws, extent[axis_at] // shards_of).reshape([-1 if axis == axis_at else 1 for axis in range(len(extent))])
    return level


def noise(own_key, shape, scale, reach, cuts=(), kind=jnp.bfloat16):
    gain = block_scale(own_key, shape, cuts, -0.22, 0.18) if cuts else 1.0
    result = jax.random.normal(own_key, shape, jnp.float32) * scale * gain
    return jnp.minimum(jnp.maximum(result, -reach), reach).astype(kind)


def setup_inputs(seed: int = 0) -> dict:
    keys = jax.random.split(jax.random.key(seed), 7)
    return {
        "tokens": noise(keys[0], (BATCH, LENGTH, D), 1.0, 6.0, ((0, 2), (1, 16))),
        "w_in": noise(keys[1], (D, PROJ), (4 * D) ** -0.5, 0.0625, ((0, 2),)),
        "a_log": jnp.clip(jax.random.uniform(keys[2], (HEADS,), jnp.float32, -8.0, 0.0), -8.0, 0.0),
        "dt_bias": jnp.clip(jax.random.uniform(keys[3], (HEADS,), jnp.float32, -4.5, -3.5), -4.5, -3.5),
        "d_skip": jnp.clip(jax.random.uniform(keys[4], (HEADS,), jnp.float32, 0.5, 1.5), 0.5, 1.5),
        "grad_y": noise(keys[5], (BATCH, LENGTH, INNER), 1.0, 6.0, ((0, 2), (1, 16))),
    }


def block_ssd(xs, bm, cm, raw, start, a_log, dt_bias, d_skip):
    high = lax.Precision.HIGHEST
    dt = jax.nn.softplus(raw + dt_bias)
    loga = -jnp.exp(a_log) * dt
    cum = jnp.cumsum(loga, axis=0)
    count = xs.shape[0]
    later = (jnp.arange(count)[:, None] >= jnp.arange(count)[None, :])[:, :, None]
    spans = cum[:, None, :] - cum[None, :, :]
    decay = jnp.where(later, jnp.exp(jnp.where(later, spans, 0.0)), 0.0)
    scores = jnp.dot(cm, bm.T, precision=high)
    mixing = scores[:, :, None] * decay * dt[None, :, :]
    ssd = jnp.einsum('tsh,shp->thp', mixing, xs, precision=high)
    ssd = ssd + jnp.einsum('tn,th,hpn->thp', cm, jnp.exp(cum), start, precision=high)
    out = ssd + d_skip[None, :, None] * xs
    tail = jnp.exp(cum[-1:] - cum) * dt
    state = jnp.exp(cum[-1])[:, None, None] * start + jnp.einsum('sh,sn,shp->hpn', tail, bm, xs, precision=high)
    return (out, state)

def reference(tokens, w_in, a_log, dt_bias, d_skip, grad_y):
    proj = jnp.dot(tokens.reshape(BATCH * LENGTH, D), w_in, preferred_element_type=jnp.float32)
    proj = proj.reshape(BATCH, LENGTH, PROJ)
    xs = lax.optimization_barrier(proj[:, :, :INNER].astype(jnp.bfloat16)).astype(jnp.float32)
    bm = lax.optimization_barrier(proj[:, :, INNER:INNER + STATE].astype(jnp.bfloat16)).astype(jnp.float32)
    cm = lax.optimization_barrier(proj[:, :, INNER + STATE:INNER + 2 * STATE].astype(jnp.bfloat16)).astype(jnp.float32)
    raw = proj[:, :, INNER + 2 * STATE:]
    blocks = LENGTH // TOK_DEV

    def forward(xseq, bseq, cseq, rseq):
        xb = xseq.reshape(blocks, TOK_DEV, HEADS, HEAD_SIZE)
        bb = bseq.reshape(blocks, TOK_DEV, STATE)
        cb = cseq.reshape(blocks, TOK_DEV, STATE)
        rb = rseq.reshape(blocks, TOK_DEV, HEADS)

        def step(carry, item):
            out, state = block_ssd(item[0], item[1], item[2], item[3], carry, a_log, dt_bias, d_skip)
            return (state, out)
        initial = jnp.zeros((HEADS, HEAD_SIZE, STATE), jnp.float32)
        final, outs = lax.scan(step, initial, (xb, bb, cb, rb))
        return outs.reshape(LENGTH, INNER)

    def one_sequence(item):
        xseq, bseq, cseq, rseq, gseq = item
        out, pullback = jax.vjp(forward, xseq, bseq, cseq, rseq)
        gx, gb, gc, gr = pullback(gseq.astype(jnp.float32))
        return (out, jnp.concatenate([gx, gb, gc, gr], axis=1))
    outs, grads = lax.map(one_sequence, (xs, bm, cm, raw, grad_y))
    y_out = outs.astype(jnp.bfloat16)
    gproj = grads.astype(jnp.bfloat16)
    grad_tokens = jnp.dot(gproj.reshape(BATCH * LENGTH, PROJ), w_in.T, preferred_element_type=jnp.float32)
    grad_tokens = grad_tokens.astype(jnp.bfloat16).reshape(BATCH, LENGTH, D)
    ublocks = tokens.reshape(BATCH * N_SEQ, TOK_DEV, D)
    gblocks = gproj.reshape(BATCH * N_SEQ, TOK_DEV, PROJ)

    def add_part(total, item):
        part = jnp.dot(item[0].T, item[1], preferred_element_type=jnp.float32)
        part = lax.optimization_barrier(part.astype(jnp.bfloat16)).astype(jnp.float32)
        return (total + part, None)
    grad_w, unused = lax.scan(add_part, jnp.zeros((D, PROJ), jnp.float32), (ublocks, gblocks))
    return (y_out, grad_tokens, grad_w)
```

```python
import jax
import jax.numpy as jnp
from jax import lax
from jax.sharding import PartitionSpec as P

BF = jnp.bfloat16
F32 = jnp.float32


def shift(value, axis, step):
    count = lax.axis_size(axis)
    return lax.ppermute(value, axis, [(i, (i + step) % count) for i in range(count)])


def flip(value, axis, bit):
    count = lax.axis_size(axis)
    return lax.ppermute(value, axis, [(i, i ^ bit) for i in range(count)])


def dot(a, b, dims):
    return lax.dot_general(a, b, (dims, ((), ())), preferred_element_type=F32)


def bdot(a, b, spec):
    return jnp.einsum(spec, a, b, preferred_element_type=F32)


def scan_states(states, totals):
    count = states.shape[0]
    fwd, bwd = states[:, :, 0].astype(F32), states[:, :, 1].astype(F32)
    run, ahead = [jnp.zeros_like(fwd[0])], [jnp.zeros_like(bwd[0])]
    for k in range(count - 1):
        run.append(jnp.exp(totals[k])[:, None, None] * run[-1] + fwd[k])
    for k in range(count - 1, 0, -1):
        ahead.append(jnp.exp(totals[k])[:, None, None] * ahead[-1] + bwd[k])
    return jnp.stack(
        [jnp.stack(run).astype(BF), jnp.stack(ahead[::-1]).astype(BF)], axis=2
    )


def ssd_block(proj, gy, a_log, dt_bias, d_skip):
    count, inner = gy.shape
    heads = a_log.shape[0]
    width = inner // heads
    size = (proj.shape[1] - inner - heads) // 2
    xs = proj[:, :inner].astype(BF)
    bm = proj[:, inner : inner + size].astype(BF)
    cm = proj[:, inner + size : inner + 2 * size].astype(BF)
    raw = proj[:, inner + 2 * size :] + dt_bias
    dt = jax.nn.softplus(raw)
    rate = -jnp.exp(a_log)
    lower = jnp.arange(count)[:, None] >= jnp.arange(count)[None, :]
    cum = jnp.dot(lower.astype(F32), rate * dt, precision=lax.Precision.HIGHEST)
    total = cum[-1]
    growth = jnp.exp(cum)
    fade = jnp.exp(total - cum)
    x3 = xs.reshape(count, heads, width).astype(F32)
    g3 = gy.reshape(count, heads, width).astype(F32)
    xd = (x3 * dt[:, :, None]).astype(BF)
    grown = (g3 * growth[:, :, None]).astype(BF).reshape(count, inner)
    faded = (xd.astype(F32) * fade[:, :, None]).astype(BF).reshape(count, inner)
    local_f = dot(faded, bm, ((0,), (0,)))
    local_g = dot(grown, cm, ((0,), (0,)))
    shape = (heads, width, size)
    pair = jnp.stack([local_f.reshape(shape), local_g.reshape(shape)], axis=1).astype(BF)

    seq = lax.axis_size("seq")
    mine = lax.axis_index("seq")
    share = heads // seq
    totals = lax.all_gather(total, "seq")
    got = lax.all_to_all(
        pair.reshape(seq, share, 2, width, size), "seq", split_axis=0, concat_axis=0, tiled=True
    )
    own = lax.dynamic_slice_in_dim(totals, mine * share, share, axis=1)
    back = lax.all_to_all(scan_states(got, own), "seq", split_axis=0, concat_axis=0, tiled=True)
    start = back[:, :, 0].reshape(inner, size)
    end = back[:, :, 1].reshape(inner, size)

    spans = cum.T[:, :, None] - cum.T[:, None, :]
    decay = jnp.where(lower[None], jnp.exp(jnp.where(lower[None], spans, 0.0)), 0.0)
    scores = dot(cm, bm, ((1,), (1,)))
    mixing = (scores[None] * decay).astype(BF)
    gb3 = gy.reshape(count, heads, width)
    y_in = bdot(mixing, xd, "hts,shp->thp")
    back_in = bdot(mixing, gb3, "hts,thp->shp")
    cross = bdot(gb3, xd, "thp,shp->hts")
    mixed = jnp.sum(cross * decay, axis=0).astype(BF)

    y3 = y_in + dot(cm, start, ((1,), (1,))).reshape(x3.shape) * growth[:, :, None]
    h3 = back_in + dot(bm, end, ((1,), (1,))).reshape(x3.shape) * fade[:, :, None]
    out = y3 + d_skip[:, None] * x3
    grad_x = h3 * dt[:, :, None] + d_skip[:, None] * g3
    grad_c = dot(mixed, bm, ((1,), (0,))) + dot(grown, start, ((1,), (0,)))
    grad_b = dot(mixed, cm, ((0,), (0,))) + dot(faded, end, ((1,), (0,)))
    row = jnp.sum(g3 * y3, axis=2)
    column = jnp.sum(xd.astype(F32) * h3, axis=2)
    grad_dt = jnp.sum(x3 * h3, axis=2)
    joint = jnp.sum((start.astype(F32) * end.astype(F32)).reshape(heads, -1), axis=1)
    tail = jnp.sum(
        xd.astype(F32) * dot(bm, end, ((1,), (1,))).reshape(x3.shape) * fade[:, :, None], axis=(0, 2)
    )
    last = tail + jnp.exp(total) * joint
    grad_log = jnp.dot(
        lower.astype(F32).T, row - column, precision=lax.Precision.HIGHEST
    ) + last
    grad_raw = (grad_dt + grad_log * rate) * jax.nn.sigmoid(raw)
    gproj = jnp.concatenate(
        [grad_x.reshape(count, inner), grad_b, grad_c, grad_raw], axis=1
    ).astype(BF)
    return out.reshape(count, inner).astype(BF), gproj


def halving(piece_sum, bits, names):
    mine = lax.axis_index("seq")
    for name in bits:
        at = names.index(name)
        bit = (mine // name) % 2
        away = lax.dynamic_index_in_dim(piece_sum, 1 - bit, at, keepdims=False)
        keep = lax.dynamic_index_in_dim(piece_sum, bit, at, keepdims=False)
        piece_sum = keep + flip(away.astype(BF), "seq", name).astype(F32)
        names = names[:at] + names[at + 1 :]
    return piece_sum


def per_device(tokens, w_in, a_log, dt_bias, d_skip, grad_y):
    count, width = tokens.shape[1:]
    inner = grad_y.shape[2]
    heads = a_log.shape[0]
    columns = w_in.shape[1]
    exact = columns - heads
    zero = lax.axis_size("zero")
    seq = lax.axis_size("seq")
    here = lax.axis_index("zero")
    place = lax.axis_index("seq")
    owned = width // zero
    rows = tokens.reshape(count, width)

    def columns_of(z):
        return lax.dynamic_slice_in_dim(rows, z * owned, owned, axis=1)

    guests = [shift(columns_of((here + s) % zero), "zero", s) for s in range(1, zero)]
    proj = jnp.dot(columns_of(here), w_in, preferred_element_type=F32)
    for s, guest in zip(range(1, zero), guests):
        part = jnp.dot(guest, w_in, preferred_element_type=F32)
        wide = shift(part[:, :exact].astype(BF), "zero", zero - s)
        narrow = shift(part[:, exact:], "zero", zero - s)
        proj = proj + jnp.concatenate([wide.astype(F32), narrow], axis=1)

    piece = width // (seq * zero)
    cut = rows.reshape(count, seq, zero, piece)

    def pieces_of(z):
        return lax.dynamic_index_in_dim(cut, z, 2, keepdims=False).reshape(count, seq * piece)

    theirs = [shift(pieces_of((here + s) % zero), "zero", s) for s in range(1, zero)]

    y_out, gproj = ssd_block(proj, grad_y.reshape(count, inner), a_log, dt_bias, d_skip)

    others = [shift(gproj, "zero", s) for s in range(1, zero)]
    mine = dot(gproj, w_in, ((1,), (1,))).astype(BF)
    grads = jnp.zeros((count, zero, owned), BF)
    grads = lax.dynamic_update_slice_in_dim(grads, mine[:, None], here, axis=1)
    for s, other in zip(range(1, zero), others):
        made = shift(dot(other, w_in, ((1,), (1,))).astype(BF), "zero", zero - s)
        grads = lax.dynamic_update_slice_in_dim(grads, made[:, None], (here + s) % zero, axis=1)
    grad_tokens = grads.reshape(1, count, width)

    left = jnp.concatenate([pieces_of(here)] + theirs, axis=0)
    right = jnp.concatenate([gproj] + others, axis=0)
    levels = seq.bit_length() - 1
    names = [1 << b for b in reversed(range(levels))]
    core = place % 2
    left = left.reshape(left.shape[0], seq // 2, 2, piece)

    def partial(core_of, span):
        chosen = lax.dynamic_index_in_dim(left, core_of, 2, keepdims=False)
        chosen = chosen.reshape(left.shape[0], seq // 2 * piece)
        return dot(chosen, right[:, span], ((0,), (0,)))

    done = []
    half = columns // 2 // 128 * 128
    rest = names[:-1]
    for span, order in (
        (slice(0, half), rest[::-1]),
        (slice(half, columns), rest[:-1][::-1] + rest[-1:]),
    ):
        swapped = flip(partial(1 - core, span).astype(BF), "seq", 1)
        summed = partial(core, span) + swapped.astype(F32)
        summed = summed.reshape([2] * (levels - 1) + [piece, summed.shape[1]])
        done.append(halving(summed, order, rest))
    grad_w = jnp.concatenate(done, axis=1)
    return (y_out.reshape(1, count, inner), grad_tokens, grad_w)


def solution(mesh):
    placed = (P("zero", "seq", None), P("zero", None), P(), P(), P(), P("zero", "seq", None))
    return jax.shard_map(
        per_device,
        mesh=mesh,
        in_specs=placed,
        out_specs=(P("zero", "seq", None), P("zero", "seq", None), P(("seq", "zero"), None)),
        check_vma=False,
    )
```

```python
import functools

import jax
import jax.numpy as jnp
from jax import lax
from jax.experimental import pallas as pl
from jax.experimental.pallas import tpu as pltpu
from jax.sharding import PartitionSpec as P

BF = jnp.bfloat16
F32 = jnp.float32
MESH = pl.DeviceIdType.MESH


def shift(value, axis, step):
    count = lax.axis_size(axis)
    return lax.ppermute(value, axis, [(i, (i + step) % count) for i in range(count)])


def dot(a, b, dims):
    return lax.dot_general(a, b, (dims, ((), ())), preferred_element_type=F32)


def bdot(a, b, spec):
    return jnp.einsum(spec, a, b, preferred_element_type=F32)


def greet(peers):
    barrier = pltpu.get_barrier_semaphore()
    for peer in peers:
        pl.semaphore_signal(barrier, inc=1, device_id={"seq": peer}, device_id_type=MESH)
    pl.semaphore_wait(barrier, len(peers))


def remote(src, dst, send, recv, peer):
    return pltpu.make_async_remote_copy(
        src_ref=src,
        dst_ref=dst,
        send_sem=send,
        recv_sem=recv,
        device_id={"seq": peer},
        device_id_type=MESH,
    )


def scan_kernel(
    pair, totals, start, end, both, marks, joined, sums, got, lengths, made, back, final, wide,
    send, recv, local
):
    chips, _, share = pair.shape[:3]
    me = lax.axis_index("seq")
    core, chip = lax.rem(me, 2), lax.div(me, 2)
    sibling = me + 1 - 2 * core
    places = [lax.rem(chip + d, chips) for d in range(1, chips)]
    peers = [place * 2 + core for place in places]
    greet([sibling] + peers)

    def move(copies):
        for copy in copies:
            copy.start()
        for copy in copies:
            copy.wait()

    move(
        [
            remote(pair.at[:, 1 - core], both.at[core], send.at[0, 0], recv.at[0, 0], sibling),
            remote(totals.at[:, 1 - core], marks.at[core], send.at[1, 0], recv.at[1, 0], sibling),
            pltpu.make_async_copy(pair.at[:, core], both.at[core], local.at[0]),
            pltpu.make_async_copy(totals.at[:, core], marks.at[core], local.at[1]),
        ]
    )

    def gain(ref, *at):
        return jnp.exp(ref[at])

    for k in range(chips):
        sums[k] = marks[0, k] + marks[1, k]
        for j in range(share):
            row = pl.ds(j, 1)
            joined[k, j, 0] = (
                gain(marks, 1, k, row) * both[0, k, j, 0].astype(F32)
                + both[1, k, j, 0].astype(F32)
            ).astype(BF)
            joined[k, j, 1] = (
                gain(marks, 0, k, row) * both[1, k, j, 1].astype(F32)
                + both[0, k, j, 1].astype(F32)
            ).astype(BF)
    copies = []
    for d, (place, peer) in enumerate(zip(places, peers)):
        copies.append(remote(joined.at[place], got.at[chip], send.at[2, d], recv.at[2, d], peer))
        copies.append(remote(sums.at[place], lengths.at[chip], send.at[3, d], recv.at[3, d], peer))
    copies.append(pltpu.make_async_copy(joined.at[chip], got.at[chip], local.at[2]))
    copies.append(pltpu.make_async_copy(sums.at[chip], lengths.at[chip], local.at[3]))
    move(copies)

    for j in range(share):
        row = pl.ds(j, 1)
        run = jnp.zeros(pair.shape[4:], F32)
        for k in range(chips):
            made[k, j, 0] = run.astype(BF)
            if k < chips - 1:
                run = gain(lengths, k, row) * run + got[k, j, 0].astype(F32)
        run = jnp.zeros(pair.shape[4:], F32)
        for k in reversed(range(chips)):
            made[k, j, 1] = run.astype(BF)
            if k > 0:
                run = gain(lengths, k, row) * run + got[k, j, 1].astype(F32)
    copies = [
        remote(made.at[place], back.at[chip], send.at[4, d], recv.at[4, d], peer)
        for d, (place, peer) in enumerate(zip(places, peers))
    ]
    move(copies + [pltpu.make_async_copy(made.at[chip], back.at[chip], local.at[4])])

    for k in range(chips):
        for j in range(share):
            row = pl.ds(j, 1)
            first, last = back[k, j, 0], back[k, j, 1]
            final[0, k, j, 0] = first
            final[1, k, j, 1] = last
            final[1, k, j, 0] = (
                gain(marks, 0, k, row) * first.astype(F32) + both[0, k, j, 0].astype(F32)
            ).astype(BF)
            final[0, k, j, 1] = (
                gain(marks, 1, k, row) * last.astype(F32) + both[1, k, j, 1].astype(F32)
            ).astype(BF)
    move(
        [
            remote(final.at[1 - core], wide.at[core], send.at[5, 0], recv.at[5, 0], sibling),
            pltpu.make_async_copy(final.at[core], wide.at[core], local.at[5]),
        ]
    )
    for parity in range(2):
        start[:, parity] = wide[parity, :, :, 0]
        end[:, parity] = wide[parity, :, :, 1]


def scan_states(pair, totals):
    chips, _, share, _, rows, lanes = pair.shape
    state = jax.ShapeDtypeStruct((chips, 2, share, rows, lanes), BF)
    half = (chips,) + pair.shape[2:]
    short = (chips,) + totals.shape[2:]
    return pl.pallas_call(
        scan_kernel,
        out_shape=(state, state),
        in_specs=[pl.BlockSpec(memory_space=pltpu.VMEM)] * 2,
        out_specs=[pl.BlockSpec(memory_space=pltpu.VMEM)] * 2,
        scratch_shapes=[
            pltpu.VMEM((2,) + half, BF),
            pltpu.VMEM((2,) + short, F32),
            pltpu.VMEM(half, BF),
            pltpu.VMEM(short, F32),
            pltpu.VMEM(half, BF),
            pltpu.VMEM(short, F32),
            pltpu.VMEM(half, BF),
            pltpu.VMEM(half, BF),
            pltpu.VMEM((2,) + half, BF),
            pltpu.VMEM((2,) + half, BF),
            pltpu.SemaphoreType.DMA((6, chips)),
            pltpu.SemaphoreType.DMA((6, chips)),
            pltpu.SemaphoreType.DMA((6,)),
        ],
        compiler_params=pltpu.CompilerParams(collective_id=0, has_side_effects=True),
    )(pair, totals)


def sum_kernel(seq, spans, tile, left, right, out, *scratch):
    levels = (seq // 2).bit_length() - 1
    me = lax.axis_index("seq")
    core, place = lax.rem(me, 2), lax.div(me, 2)
    bits = [lax.rem(lax.div(place, 1 << b), 2) for b in range(levels)]
    sibling = me + 1 - 2 * core
    partners = [me + (1 - 2 * bits[b]) * (2 << b) for b in range(levels)]
    greet([sibling] + partners)
    pieces, piece, tokens = left.shape[1:]
    parts = len(spans)
    up = list(range(levels))
    orders = [up, up[1:] + up[:1]] * (parts // 2)
    acc, away, come = (scratch[i * parts : (i + 1) * parts] for i in range(3))
    rest = scratch[3 * parts : -2]
    outs = [rest[h * levels : (h + 1) * levels] for h in range(parts)]
    ins = [rest[(parts + h) * levels : (parts + h + 1) * levels] for h in range(parts)]
    send, recv = scratch[-2:]

    def multiply(side, h, target):
        low, high = spans[h]
        rows = left[side].reshape(pieces * piece, tokens)
        full = (high - low) // tile

        def column(first, own, wide):
            made = jnp.dot(rows, right[:, pl.ds(first, wide)], preferred_element_type=F32)
            target[:, :, pl.ds(own, wide)] = made.reshape(pieces, piece, wide).astype(target.dtype)

        @pl.loop(0, full)
        def _(i):
            own = pl.multiple_of(i * tile, 128)
            column(pl.multiple_of(low + i * tile, 128), own, tile)

        if (high - low) % tile:
            column(low + full * tile, full * tile, (high - low) % tile)

    first = []
    for h in range(parts):
        multiply(1 - core, h, away[h])
        copy = remote(away[h], come[h], send.at[h, levels], recv.at[h, levels], sibling)
        copy.start()
        first.append(copy)

    def subsets(rest):
        found = [0]
        for b in rest:
            found = found + [value + (1 << b) for value in found]
        return found

    def begin(h, s):
        order = orders[h]
        b = order[s]
        base = sum((bits[f] * (1 << f) for f in order[:s]), 0)
        for j, extra in enumerate(subsets(order[s + 1 :])):
            outs[h][s][j] = acc[h][base + (1 - bits[b]) * (1 << b) + extra].astype(BF)
        copy = remote(outs[h][s], ins[h][s], send.at[h, s], recv.at[h, s], partners[b])
        copy.start()
        return copy

    def finish(h, s, copy):
        copy.wait()
        order = orders[h]
        base = sum((bits[f] * (1 << f) for f in order[: s + 1]), 0)
        for j, extra in enumerate(subsets(order[s + 1 :])):
            acc[h][base + extra] += ins[h][s][j].astype(F32)

    flying = []
    for h in range(parts):
        multiply(core, h, acc[h])
        first[h].wait()

        @pl.loop(0, pieces)
        def _(i):
            acc[h][i] += come[h][i].astype(F32)

        flying.append(begin(h, 0))
    for s in range(levels):
        for h in range(parts):
            finish(h, s, flying[h])
            if s + 1 < levels:
                flying[h] = begin(h, s + 1)
    for h in range(parts):
        out[:, spans[h][0] : spans[h][1]] = acc[h][place]


def sum_shards(left, right):
    pieces, piece = left.shape[1:3]
    cols = right.shape[1]
    seq = 2 * pieces
    tile, parts = 256, 4
    levels = pieces.bit_length() - 1
    edges = [(2 * i * cols // parts + 128) // 256 * 128 for i in range(parts)] + [cols]
    spans = list(zip(edges[:-1], edges[1:]))
    widths = [high - low for low, high in spans]
    scratch = [pltpu.VMEM((pieces, piece, w), F32) for w in widths]
    scratch += [pltpu.VMEM((pieces, piece, w), BF) for w in widths] * 2
    for _ in range(2):
        for w in widths:
            scratch += [pltpu.VMEM((pieces >> (s + 1), piece, w), BF) for s in range(levels)]
    scratch += [pltpu.SemaphoreType.DMA((parts, levels + 1))] * 2
    return pl.pallas_call(
        functools.partial(sum_kernel, seq, spans, tile),
        out_shape=jax.ShapeDtypeStruct((piece, cols), F32),
        in_specs=[pl.BlockSpec(memory_space=pltpu.VMEM)] * 2,
        out_specs=pl.BlockSpec(memory_space=pltpu.VMEM),
        scratch_shapes=scratch,
        compiler_params=pltpu.CompilerParams(collective_id=1, has_side_effects=True),
    )(left, right)


def ssd_block(proj, gy, a_log, dt_bias, d_skip):
    count, inner = gy.shape
    heads = a_log.shape[0]
    width = inner // heads
    size = (proj.shape[1] - inner - heads) // 2
    xs = proj[:, :inner].astype(BF)
    bm = proj[:, inner : inner + size].astype(BF)
    cm = proj[:, inner + size : inner + 2 * size].astype(BF)
    raw = proj[:, inner + 2 * size :] + dt_bias
    dt = jax.nn.softplus(raw)
    rate = -jnp.exp(a_log)
    lower = jnp.arange(count)[:, None] >= jnp.arange(count)[None, :]
    cum = jnp.dot(lower.astype(F32), rate * dt, precision=lax.Precision.HIGHEST)
    total = cum[-1]
    growth = jnp.exp(cum)
    fade = jnp.exp(total - cum)
    x3 = xs.reshape(count, heads, width).astype(F32)
    g3 = gy.reshape(count, heads, width).astype(F32)
    xd = (x3 * dt[:, :, None]).astype(BF)
    grown = (g3 * growth[:, :, None]).astype(BF).reshape(count, inner)
    faded = (xd.astype(F32) * fade[:, :, None]).astype(BF).reshape(count, inner)
    local_f = dot(faded, bm, ((0,), (0,)))
    local_g = dot(grown, cm, ((0,), (0,)))
    shape = (heads, width, size)
    pair = jnp.stack([local_f.reshape(shape), local_g.reshape(shape)], axis=1).astype(BF)

    seq = lax.axis_size("seq")
    share = heads // seq
    marks = jnp.pad(total.reshape(seq, share), ((0, 0), (0, -share % 8)))
    marks = jnp.broadcast_to(marks[:, :, None], marks.shape + (size,))
    marks = marks.reshape(seq // 2, 2, -1, size)
    start, end = scan_states(pair.reshape(seq // 2, 2, share, 2, width, size), marks)
    start, end = start.reshape(inner, size), end.reshape(inner, size)

    spans = cum.T[:, :, None] - cum.T[:, None, :]
    decay = jnp.where(lower[None], jnp.exp(jnp.where(lower[None], spans, 0.0)), 0.0)
    scores = dot(cm, bm, ((1,), (1,)))
    mixing = (scores[None] * decay).astype(BF)
    gb3 = gy.reshape(count, heads, width)
    y_in = bdot(mixing, xd, "hts,shp->thp")
    back_in = bdot(mixing, gb3, "hts,thp->shp")
    cross = bdot(gb3, xd, "thp,shp->hts")
    mixed = jnp.sum(cross * decay, axis=0).astype(BF)

    y3 = y_in + dot(cm, start, ((1,), (1,))).reshape(x3.shape) * growth[:, :, None]
    h3 = back_in + dot(bm, end, ((1,), (1,))).reshape(x3.shape) * fade[:, :, None]
    out = y3 + d_skip[:, None] * x3
    grad_x = h3 * dt[:, :, None] + d_skip[:, None] * g3
    grad_c = dot(mixed, bm, ((1,), (0,))) + dot(grown, start, ((1,), (0,)))
    grad_b = dot(mixed, cm, ((0,), (0,))) + dot(faded, end, ((1,), (0,)))
    row = jnp.sum(g3 * y3, axis=2)
    column = jnp.sum(xd.astype(F32) * h3, axis=2)
    grad_dt = jnp.sum(x3 * h3, axis=2)
    joint = jnp.sum((start.astype(F32) * end.astype(F32)).reshape(heads, -1), axis=1)
    tail = jnp.sum(
        xd.astype(F32) * dot(bm, end, ((1,), (1,))).reshape(x3.shape) * fade[:, :, None], axis=(0, 2)
    )
    last = tail + jnp.exp(total) * joint
    grad_log = jnp.dot(
        lower.astype(F32).T, row - column, precision=lax.Precision.HIGHEST
    ) + last
    grad_raw = (grad_dt + grad_log * rate) * jax.nn.sigmoid(raw)
    gproj = jnp.concatenate(
        [grad_x.reshape(count, inner), grad_b, grad_c, grad_raw], axis=1
    ).astype(BF)
    return out.reshape(count, inner).astype(BF), gproj


def per_device(tokens, w_in, a_log, dt_bias, d_skip, grad_y):
    count, width = tokens.shape[1:]
    inner = grad_y.shape[2]
    heads = a_log.shape[0]
    columns = w_in.shape[1]
    exact = columns - heads
    zero = lax.axis_size("zero")
    seq = lax.axis_size("seq")
    here = lax.axis_index("zero")
    owned = width // zero
    rows = tokens.reshape(count, width)

    def columns_of(z):
        return lax.dynamic_slice_in_dim(rows, z * owned, owned, axis=1)

    guests = [shift(columns_of((here + s) % zero), "zero", s) for s in range(1, zero)]
    proj = jnp.dot(columns_of(here), w_in, preferred_element_type=F32)
    for s, guest in zip(range(1, zero), guests):
        part = jnp.dot(guest, w_in, preferred_element_type=F32)
        wide = shift(part[:, :exact].astype(BF), "zero", zero - s)
        narrow = shift(part[:, exact:], "zero", zero - s)
        proj = proj + jnp.concatenate([wide.astype(F32), narrow], axis=1)

    piece = width // (seq * zero)
    cut = rows.reshape(count, seq, zero, piece)

    def pieces_of(z):
        return lax.dynamic_index_in_dim(cut, z, 2, keepdims=False).reshape(count, seq * piece)

    theirs = [shift(pieces_of((here + s) % zero), "zero", s) for s in range(1, zero)]

    y_out, gproj = ssd_block(proj, grad_y.reshape(count, inner), a_log, dt_bias, d_skip)

    others = [shift(gproj, "zero", s) for s in range(1, zero)]
    mine = dot(gproj, w_in, ((1,), (1,))).astype(BF)
    grads = [mine]
    for s, other in zip(range(1, zero), others):
        grads.append(shift(dot(other, w_in, ((1,), (1,))).astype(BF), "zero", zero - s))
    blocks = []
    for z in range(zero):
        block = grads[0]
        for s in range(1, zero):
            block = jnp.where((here + s) % zero == z, grads[s], block)
        blocks.append(block)
    grad_tokens = jnp.concatenate(blocks, axis=1).reshape(1, count, width)

    left = jnp.concatenate([pieces_of(here)] + theirs, axis=0)
    right = jnp.concatenate([gproj] + others, axis=0)
    left = left.reshape(left.shape[0], seq // 2, 2, piece).transpose(2, 1, 3, 0)
    grad_w = sum_shards(left, right)
    return (y_out.reshape(1, count, inner), grad_tokens, grad_w)


def solution(mesh):
    placed = (P("zero", "seq", None), P("zero", None), P(), P(), P(), P("zero", "seq", None))
    return jax.shard_map(
        per_device,
        mesh=mesh,
        in_specs=placed,
        out_specs=(P("zero", "seq", None), P("zero", "seq", None), P(("seq", "zero"), None)),
        check_vma=False,
    )
```
